256 devices in a mesh: snap: 8 (over z), vert: 32 (over x, y, core).
Axes of the slice: x: 4, y: 4, z: 8, core: 2. Of those that a mesh axis runs over, the one named last changes fastest.
Arguments:
- features: bfloat16 [16, 65536, 256], P('snap', 'vert'), may hold values from -6 to 6
- tile_rows: int32 [16, 2048], P('snap', 'vert'), may hold values from 0 to 15
- tile_cols: int32 [16, 2048], P('snap', 'vert'), may hold values from 0 to 21
- tile_vals: bfloat16 [16, 2048, 128, 128], P('snap', 'vert'), may hold values from -0.25 to 0.25
- send_lists: int32 [32, 6], replicated, may hold values from 0 to 15
- conv1_weight: bfloat16 [256, 256], replicated, may hold values from -0.375 to 0.375
- conv2_weight: bfloat16 [256, 256], replicated, may hold values from -0.375 to 0.375
- lstm_weight: bfloat16 [2, 512, 1024], replicated, may hold values from -0.25 to 0.25
- lstm_bias: float32 [2, 1024], replicated, may hold values from -4 to 4
Outputs:
- mixed: bfloat16 [16, 65536, 256], P('snap', 'vert')
The draws below stay inside these ranges and needn't reach their ends.
All inputs are finite; a program needn't handle non-finite values.
Results may differ from the reference program's by a relative error of at most 0.007.
Values may be sent and summed in bfloat16 or wider, within the bound.
A program may use at most 128 MiB of HBM per device.

```python
import jax
import jax.numpy as jnp
from jax import lax

F = 256
BS = 128
BND = 3
BLK_DEV = 16
TILE_DEV = 64
SNAPS = 16
VERTS = 65536
TILES = 2048
N_VERT = 32


def plant(drawn, stream_key, smallest, high):
    shape = drawn.shape
    place = [jax.random.randint(jax.random.fold_in(stream_key, axis), (), 0, shape[axis]) for axis in range(len(shape))]
    drawn = drawn.at[tuple(place)].set(smallest)
    longest = shape.index(max(shape))
    place[longest] = (place[longest] + 1) % shape[longest]
    return drawn.at[tuple(place)].set(high)


def block_scale(stream_key, shape, shards, smallest, top_value):
    def one(dim, shards_of):
        heights = jax.random.uniform(jax.random.fold_in(jax.random.fold_in(stream_key, 6), dim), (shards_of,), jnp.float32, smallest / len(shards), top_value / len(shards))
        return jnp.repeat(jnp.exp(heights), shape[dim] // shards_of).reshape((-1,) + (1,) * (len(shape) - dim - 1))

    gain = one(*shards[0])
    for cut in shards[1:]:
        gain = gain * one(*cut)
    return gain


def gaussian(rng, dims, width, bound, cuts=(), kind=jnp.bfloat16):
    array = jax.random.normal(rng, dims, jnp.float32) * width
    if len(cuts) > 0:
        array = block_scale(rng, dims, cuts, -0.22, 0.18) * array
    return jnp.clip(array, min=-bound, max=bound).astype(kind)


def setup_inputs(seed: int = 0) -> dict:
    key_list = jax.random.split(jax.random.key(seed), 10)
    features = gaussian(key_list[0], (SNAPS, VERTS, F), 1.0, 6.0, ((0, 8), (1, 32)))
    tile_rows = plant(jax.random.randint(key_list[1], (SNAPS, TILES), 0, BLK_DEV), jax.random.fold_in(key_list[1], 1), 0, BLK_DEV - 1).astype(jnp.int32)
    tile_cols = plant(jax.random.randint(key_list[2], (SNAPS, TILES), 0, BLK_DEV + 2 * BND), jax.random.fold_in(key_list[2], 1), 0, (BLK_DEV + 2 * BND) - 1).astype(jnp.int32)
    tile_vals = gaussian(key_list[3], (SNAPS, TILES, BS, BS), (BS * max(TILE_DEV // BLK_DEV, 1)) ** -0.5, 0.25, ((0, 8), (1, 32)))
    send_lists = plant(jax.random.randint(key_list[4], (N_VERT, 2 * BND), 0, BLK_DEV), jax.random.fold_in(key_list[4], 1), 0, BLK_DEV - 1).astype(jnp.int32)
    conv1_weight = gaussian(key_list[5], (F, F), F ** -0.5, 0.375)
    conv2_weight = gaussian(key_list[6], (F, F), F ** -0.5, 0.375)
    lstm_weight = gaussian(key_list[7], (2, 2 * F, 4 * F), (2 * F) ** -0.5, 0.25)
    lstm_bias = gaussian(key_list[8], (2, 4 * F), 1.0, 4.0, (), jnp.float32)
    return {"features": features, "tile_rows": tile_rows, "tile_cols": tile_cols, "tile_vals": tile_vals, "send_lists": send_lists, "conv1_weight": conv1_weight, "conv2_weight": conv2_weight, "lstm_weight": lstm_weight, "lstm_bias": lstm_bias}


def convolve(field, tile_rows, tile_cols, tile_vals, send_lists):
    left_list = jnp.roll(send_lists, 1, axis=0)[:, BND:].astype(jnp.int32)
    right_list = jnp.roll(send_lists, -1, axis=0)[:, :BND].astype(jnp.int32)

    def single(packed):
        slab, rows_t, cols_t, vals_t = packed
        blocks = slab.reshape(N_VERT, BLK_DEV, BS, F)
        left = jnp.take_along_axis(jnp.roll(blocks, 1, axis=0), left_list[:, :, None, None], axis=1)
        right = jnp.take_along_axis(jnp.roll(blocks, -1, axis=0), right_list[:, :, None, None], axis=1)
        extended = jnp.concatenate([left, blocks, right], axis=1)
        picked = jnp.take_along_axis(extended, cols_t.reshape(N_VERT, TILE_DEV)[:, :, None, None].astype(jnp.int32), axis=1)
        values = vals_t.reshape(N_VERT, TILE_DEV, BS, BS)
        product = jnp.einsum("dkij,dkjf->dkif", values.astype(jnp.float32), picked.astype(jnp.float32), precision=lax.Precision.HIGHEST)
        onehot = (rows_t.reshape(N_VERT, TILE_DEV)[:, :, None] == jnp.arange(BLK_DEV, dtype=jnp.int32)).astype(jnp.float32)
        summed = jnp.einsum("dkb,dkif->dbif", onehot, product, precision=lax.Precision.HIGHEST)
        return summed.reshape(N_VERT * BLK_DEV * BS, F)

    return lax.map(single, (field, tile_rows, tile_cols, tile_vals))


def project(field, weight):
    return jnp.einsum("svf,fg->svg", field.astype(jnp.float32), weight.astype(jnp.float32), precision=lax.Precision.HIGHEST).astype(jnp.bfloat16)


def cell_step(inputs, hidden, memory, weight, bias):
    gates = jnp.dot(jnp.concatenate([inputs, hidden], axis=-1), weight, preferred_element_type=jnp.float32) + bias
    in_gate, forget, candidate, out_gate = jnp.split(gates, 4, axis=-1)
    memory = jax.nn.sigmoid(forget) * memory + jax.nn.sigmoid(in_gate) * jnp.tanh(candidate)
    hidden = (jax.nn.sigmoid(out_gate) * jnp.tanh(memory)).astype(jnp.bfloat16)
    return hidden, memory


def recurrence(sequence, lstm_weight, lstm_bias):
    count = sequence.shape[1]
    zero_h = jnp.zeros((count, F), jnp.bfloat16)
    zero_c = jnp.zeros((count, F), jnp.float32)

    def advance(carry, inputs):
        first_h, first_c, second_h, second_c = carry
        first_h, first_c = cell_step(inputs, first_h, first_c, lstm_weight[0], lstm_bias[0])
        second_h, second_c = cell_step(first_h, second_h, second_c, lstm_weight[1], lstm_bias[1])
        return (first_h, first_c, second_h, second_c), second_h

    carry, outputs = lax.scan(advance, (zero_h, zero_c, zero_h, zero_c), sequence)
    return outputs


def reference(features, tile_rows, tile_cols, tile_vals, send_lists, conv1_weight, conv2_weight, lstm_weight, lstm_bias):
    projected = project(features, conv1_weight)
    convolved = jnp.maximum(convolve(projected, tile_rows, tile_cols, tile_vals, send_lists), 0.0).astype(jnp.bfloat16)
    recurrent = recurrence(convolved, lstm_weight, lstm_bias)
    second = project(recurrent, conv2_weight)
    return convolve(second, tile_rows, tile_cols, tile_vals, send_lists).astype(jnp.bfloat16)
```

```python
import functools

import jax
import jax.numpy as jnp
from jax import lax
from jax.experimental import pallas as pl
from jax.experimental.pallas import tpu as pltpu
from jax.sharding import PartitionSpec as P

BS = 128
MESH = pl.DeviceIdType.MESH
UNROLL = 8


def conv_kernel(project, relu, rows, cols, own, halo, vals, *rest):
    if project:
        weight, out, extended, acc = rest
    else:
        out, extended, acc = rest
    snap = pl.program_id(0)
    blocks = own.shape[1]
    bound = halo.shape[2]

    def put(slot, block):
        if project:
            block = jnp.dot(block, weight[...], preferred_element_type=jnp.float32)
        extended[slot] = block.astype(jnp.bfloat16)

    for i in range(bound):
        put(i, halo[0, 0, i])
        put(bound + blocks + i, halo[1, 0, i])
    for i in range(blocks):
        put(bound + i, own[0, i])
    acc[...] = jnp.zeros_like(acc)

    def group(g, carry):
        products = []
        for u in range(UNROLL):
            k = g * UNROLL + u
            products.append(
                jnp.dot(vals[0, k], extended[cols[snap, k]], preferred_element_type=jnp.float32)
            )
        for u in range(UNROLL):
            row = rows[snap, g * UNROLL + u]
            acc[row] += products[u]
        return carry

    lax.fori_loop(0, vals.shape[1] // UNROLL, group, 0)
    for i in range(blocks):
        total = acc[i]
        if relu:
            total = jnp.maximum(total, 0.0)
        out[0, i] = total.astype(jnp.bfloat16)


def convolve(own, halo, tile_rows, tile_cols, tile_vals, weight, relu):
    snaps, blocks, _, width = own.shape
    bound = halo.shape[2]
    tiles = tile_vals.shape[1]
    project = weight is not None
    in_specs = [
        pl.BlockSpec((1, blocks, BS, width), lambda s, r, c: (s, 0, 0, 0)),
        pl.BlockSpec((2, 1, bound, BS, width), lambda s, r, c: (0, s, 0, 0, 0)),
        pl.BlockSpec((1, tiles, BS, BS), lambda s, r, c: (s, 0, 0, 0)),
    ]
    operands = [own, halo, tile_vals]
    if project:
        in_specs.append(pl.BlockSpec((width, width), lambda s, r, c: (0, 0)))
        operands.append(weight)
    return pl.pallas_call(
        functools.partial(conv_kernel, project, relu),
        out_shape=jax.ShapeDtypeStruct(own.shape, jnp.bfloat16),
        grid_spec=pltpu.PrefetchScalarGridSpec(
            num_scalar_prefetch=2,
            grid=(snaps,),
            in_specs=in_specs,
            out_specs=pl.BlockSpec((1, blocks, BS, width), lambda s, r, c: (s, 0, 0, 0)),
            scratch_shapes=[
                pltpu.VMEM((blocks + 2 * bound, BS, width), jnp.bfloat16),
                pltpu.VMEM((blocks, BS, width), jnp.float32),
            ],
        ),
        compiler_params=pltpu.CompilerParams(dimension_semantics=("arbitrary",)),
        cost_estimate=pl.CostEstimate(
            flops=2 * snaps * tiles * BS * BS * width, bytes_accessed=8 << 20, transcendentals=0
        ),
        name="conv_project" if project else "conv_plain",
    )(tile_rows, tile_cols, *operands)


def exchange(blocks, send_lists):
    count = lax.axis_size("vert")
    bound = send_lists.shape[1] // 2
    own_list = lax.dynamic_index_in_dim(send_lists, lax.axis_index("vert"), 0, keepdims=False)
    packed = jnp.take(blocks, own_list, axis=1)
    forward = [(i, (i + 1) % count) for i in range(count)]
    backward = [(target, source) for source, target in forward]
    low = lax.ppermute(packed[:, bound:], "vert", forward)
    high = lax.ppermute(packed[:, :bound], "vert", backward)
    return jnp.stack([low, high])


def sigmoid(x):
    return 0.5 * jnp.tanh(0.5 * x) + 0.5


def recur_kernel(
    n, conv, lstm_w, bias, proj_w, out,
    xbuf, hbuf, rbuf, h0, c0, h1, c1, send1, recv1, send2, recv2,
):
    me = lax.axis_index("snap")
    width = conv.shape[-1]
    offsets = [4, 3, 5, 2, 6, 1, 7] if n == 8 else list(range(1, n))

    barrier = pltpu.get_barrier_semaphore()
    for d in range(1, n):
        pl.semaphore_signal(
            barrier, inc=1, device_id={"snap": lax.rem(me + d, n)}, device_id_type=MESH
        )
    pl.semaphore_wait(barrier, n - 1)

    def first_copy(half, peer):
        return pltpu.make_async_remote_copy(
            src_ref=conv.at[:, 2 * peer + half],
            dst_ref=xbuf.at[half, pl.ds(2 * me, 2)],
            send_sem=send1.at[half, peer],
            recv_sem=recv1.at[half, me],
            device_id={"snap": peer},
            device_id_type=MESH,
        )

    for half in range(2):
        for d in offsets:
            first_copy(half, lax.rem(me + d, n)).start()
        pltpu.make_async_copy(
            conv.at[:, 2 * me + half], xbuf.at[half, pl.ds(2 * me, 2)], recv1.at[half, me]
        ).start()

    def cell(x, hidden, memory, layer):
        gates = (
            jnp.dot(x, lstm_w[layer, :width], preferred_element_type=jnp.float32)
            + jnp.dot(hidden[...], lstm_w[layer, width:], preferred_element_type=jnp.float32)
            + bias[layer][None, :]
        )
        kept = sigmoid(gates[:, width : 2 * width]) * memory[...]
        new = kept + sigmoid(gates[:, :width]) * jnp.tanh(gates[:, 2 * width : 3 * width])
        memory[...] = new
        result = (sigmoid(gates[:, 3 * width :]) * jnp.tanh(new)).astype(jnp.bfloat16)
        hidden[...] = result
        return result

    def second_copy(half, t, owner):
        return pltpu.make_async_remote_copy(
            src_ref=hbuf.at[half, t],
            dst_ref=rbuf.at[lax.rem(t, 2), 2 * me + half],
            send_sem=send2.at[half, t],
            recv_sem=recv2.at[half, lax.rem(t, 2), me],
            device_id={"snap": owner},
            device_id_type=MESH,
        )

    for half in range(2):
        h0[...] = jnp.zeros_like(h0)
        h1[...] = jnp.zeros_like(h1)
        c0[...] = jnp.zeros_like(c0)
        c1[...] = jnp.zeros_like(c1)

        def step(owner, carry, half=half):
            landed = xbuf.at[half, pl.ds(2 * owner, 2)]
            pltpu.make_async_copy(landed, landed, recv1.at[half, owner]).wait()
            for part in range(2):
                t = 2 * owner + part
                low = cell(xbuf[half, t], h0, c0, 0)
                hbuf[half, t] = cell(low, h1, c1, 1)

                @pl.when(owner != me)
                def _():
                    second_copy(half, t, owner).start()

                @pl.when(owner == me)
                def _():
                    pltpu.make_async_copy(
                        hbuf.at[half, t], rbuf.at[part, 2 * me + half], recv2.at[half, part, me]
                    ).start()

            return carry

        lax.fori_loop(0, n, step, 0)

    for part in range(2):
        for half in range(2):

            def finish(i, carry, half=half, part=part):
                source = lax.rem(me + i, n)
                slot = rbuf.at[part, 2 * source + half]
                pltpu.make_async_copy(slot, slot, recv2.at[half, part, source]).wait()
                out[part, 2 * source + half] = jnp.dot(
                    rbuf[part, 2 * source + half], proj_w[...], preferred_element_type=jnp.float32
                ).astype(jnp.bfloat16)
                return carry

            lax.fori_loop(0, n, finish, 0)

    for half in range(2):

        def drain(i, carry, half=half):
            peer = lax.rem(me + i, n)
            first_copy(half, peer).wait_send()
            for part in range(2):
                second_copy(half, 2 * peer + part, peer).wait_send()
            return carry

        lax.fori_loop(1, n, drain, 0)


def recur(convolved, lstm_weight, lstm_bias, proj_weight):
    n = lax.axis_size("snap")
    snaps, blocks, _, width = convolved.shape
    total = snaps * n
    vmem = pl.BlockSpec(memory_space=pltpu.VMEM)
    return pl.pallas_call(
        functools.partial(recur_kernel, n),
        out_shape=jax.ShapeDtypeStruct(convolved.shape, jnp.bfloat16),
        in_specs=[vmem] * 4,
        out_specs=vmem,
        scratch_shapes=[
            pltpu.VMEM((2, total, BS, width), jnp.bfloat16),
            pltpu.VMEM((2, total, BS, width), jnp.bfloat16),
            pltpu.VMEM((2, blocks, BS, width), jnp.bfloat16),
            pltpu.VMEM((BS, width), jnp.bfloat16),
            pltpu.VMEM((BS, width), jnp.float32),
            pltpu.VMEM((BS, width), jnp.bfloat16),
            pltpu.VMEM((BS, width), jnp.float32),
            pltpu.SemaphoreType.DMA((2, n)),
            pltpu.SemaphoreType.DMA((2, n)),
            pltpu.SemaphoreType.DMA((2, total)),
            pltpu.SemaphoreType.DMA((2, 2, n)),
        ],
        compiler_params=pltpu.CompilerParams(collective_id=0, has_side_effects=True),
        cost_estimate=pl.CostEstimate(
            flops=9 << 30, bytes_accessed=6 << 20, transcendentals=42 << 20
        ),
        name="recur",
    )(convolved, lstm_weight, lstm_bias, proj_weight)


def shards(
    features,
    tile_rows,
    tile_cols,
    tile_vals,
    send_lists,
    conv1_weight,
    conv2_weight,
    lstm_weight,
    lstm_bias,
):
    snapshots, vertices, width = features.shape
    own = features.reshape(snapshots, vertices // BS, BS, width)
    halo = exchange(own, send_lists)
    convolved = convolve(own, halo, tile_rows, tile_cols, tile_vals, conv1_weight, True)
    second = recur(convolved, lstm_weight, lstm_bias, conv2_weight)
    halo = exchange(second, send_lists)
    mixed = convolve(second, halo, tile_rows, tile_cols, tile_vals, None, False)
    return mixed.reshape(snapshots, vertices, width)


def solution(mesh):
    placed = (
        P("snap", "vert", None),
        P("snap", "vert"),
        P("snap", "vert"),
        P("snap", "vert", None, None),
        P(),
        P(),
        P(),
        P(),
        P(),
    )
    return jax.shard_map(
        shards, mesh=mesh, in_specs=placed, out_specs=P("snap", "vert", None), check_vma=False
    )
```

```python
import functools

import jax
import jax.numpy as jnp
from jax import lax
from jax.experimental import pallas as pl
from jax.experimental.pallas import tpu as pltpu
from jax.sharding import PartitionSpec as P

BS = 128
MESH = pl.DeviceIdType.MESH
UNROLL = 8
ORDER, COLUMN, KEEP, LAST = range(4)


def sigmoid(x):
    return 0.5 * jnp.tanh(0.5 * x) + 0.5


def whole_kernel(
    n, lists_hbm, rows_hbm, cols_hbm, features, vals, w1, w2, lstm_w, lstm_b, out,
    lists, rows, cols, ranks, table, feat0, feat1, tile0, tile1,
    ext0, ext1, ext2, ext3, pack0, pack1, pack2, pack3, running, conv, xbuf, hbuf, back0, back1, stage,
    weights1, weights2, weights, bias, h0, c0, h1, c1,
    load, store, tiny_sem, sort_sem, halo_send, halo_recv,
    send_even, send_odd, send_rest, recv_even, recv_odd, recv_rest, send_back, recv_back,
):
    me = lax.axis_index("snap")
    vert = lax.axis_index("vert")
    verts = lax.axis_size("vert")
    lower, higher = lax.rem(vert + verts - 1, verts), lax.rem(vert + 1, verts)
    blocks, width = conv.shape[1], conv.shape[-1]
    bound = lists.shape[0] // 2
    tiles = vals.shape[1]
    offsets = [4, 3, 5, 2, 6, 1, 7] if n == 8 else list(range(1, n))

    tiny = [
        pltpu.make_async_copy(a, b, tiny_sem.at[i])
        for i, (a, b) in enumerate(((lists_hbm, lists), (rows_hbm, rows), (cols_hbm, cols)))
    ]
    for copy in tiny:
        copy.start()
    sources = [w1, features.at[0], features.at[1], vals.at[0], vals.at[1], lstm_w, lstm_b, w2]
    targets = [weights1, feat0, feat1, tile0, tile1, weights, bias, weights2]
    loads = [pltpu.make_async_copy(a, b, load.at[i]) for i, (a, b) in enumerate(zip(sources, targets))]
    for copy in loads:
        copy.start()

    barrier = pltpu.get_barrier_semaphore()
    for d in range(1, n):
        pl.semaphore_signal(
            barrier, inc=1, device_id={"snap": lax.rem(me + d, n)}, device_id_type=MESH
        )
    for side in (lower, higher):
        pl.semaphore_signal(barrier, inc=1, device_id={"vert": side}, device_id_type=MESH)

    def project(block, weight):
        return jnp.dot(block, weight[...], preferred_element_type=jnp.float32).astype(jnp.bfloat16)

    def make_pack(source, weight, pack):
        for i in range(2 * bound):
            pack[i] = project(source[lists[i, vert]], weight)

    def halo_copies(pack, extended, index):
        down = pltpu.make_async_remote_copy(
            src_ref=pack.at[pl.ds(0, bound)],
            dst_ref=extended.at[pl.ds(bound + blocks, bound)],
            send_sem=halo_send.at[index, 0],
            recv_sem=halo_recv.at[index, 0],
            device_id={"vert": lower},
            device_id_type=MESH,
        )
        up = pltpu.make_async_remote_copy(
            src_ref=pack.at[pl.ds(bound, bound)],
            dst_ref=extended.at[pl.ds(0, bound)],
            send_sem=halo_send.at[index, 1],
            recv_sem=halo_recv.at[index, 1],
            device_id={"vert": higher},
            device_id_type=MESH,
        )
        return (down, up)

    def project_own(source, weight, extended):
        def some(g, carry):
            for u in range(4):
                i = 4 * g + u
                extended[bound + i] = project(source[i], weight)
            return carry

        lax.fori_loop(0, blocks // 4, some, 0)

    def convolve(s, extended, tile, finish):
        def group(g, carry):
            products = []
            for u in range(UNROLL):
                k = g * UNROLL + u
                products.append(
                    jnp.dot(
                        tile[table[4 * s + ORDER, k]],
                        extended[table[4 * s + COLUMN, k]],
                        preferred_element_type=jnp.float32,
                    )
                )
            total = running[g * UNROLL]
            for u in range(UNROLL):
                k = g * UNROLL + u
                total = total * table[4 * s + KEEP, k].astype(jnp.float32) + products[u]
                running[k + 1] = total
            return carry

        lax.fori_loop(0, tiles // UNROLL, group, 0)

        def row(g, carry):
            for u in range(4):
                r = 4 * g + u
                finish(r, running[table[4 * s + LAST, r]])
            return carry

        lax.fori_loop(0, blocks // 4, row, 0)

    def cross(source, slot, send, recv, peer):
        return pltpu.make_async_remote_copy(
            src_ref=source,
            dst_ref=slot,
            send_sem=send.at[peer],
            recv_sem=recv.at[me],
            device_id={"snap": peer},
            device_id_type=MESH,
        )

    def even_copy(peer):
        return cross(conv.at[0, 2 * peer], xbuf.at[0, 2 * me], send_even, recv_even, peer)

    def odd_copy(peer):
        return cross(conv.at[1, 2 * peer], xbuf.at[0, 2 * me + 1], send_odd, recv_odd, peer)

    def rest_copy(peer):
        return cross(
            conv.at[:, 2 * peer + 1], xbuf.at[1, pl.ds(2 * me, 2)], send_rest, recv_rest, peer
        )

    def landed(slot, semaphore):
        pltpu.make_async_copy(slot, slot, semaphore).wait()

    def sort_tiles():
        shape = (tiles, ranks.shape[1])
        lane = lax.broadcasted_iota(jnp.int32, shape, 1)
        sub = lax.broadcasted_iota(jnp.int32, shape, 0)
        square = (tiles, tiles)
        lane_sq = lax.broadcasted_iota(jnp.int32, square, 1)
        sub_sq = lax.broadcasted_iota(jnp.int32, square, 0)

        def upright(line):
            wide = jnp.broadcast_to(line, square)
            return jnp.sum(jnp.where(lane_sq == sub_sq, wide, 0), axis=1, keepdims=True)

        def pick(column, chosen):
            return jnp.sum(jnp.where(chosen, column, 0), axis=0, keepdims=True)

        for s in range(rows.shape[0]):
            row_line = rows[s : s + 1, :]
            row = upright(row_line)
            key_line = jnp.broadcast_to(row_line, square) * tiles + lane_sq
            smaller = jnp.where(key_line < row * tiles + sub_sq, 1, 0)
            rank = jnp.sum(smaller, axis=1, keepdims=True)
            chosen = rank == lane
            ranks[4 * s + ORDER : 4 * s + ORDER + 1, :] = pick(sub, chosen)
            ranks[4 * s + COLUMN : 4 * s + COLUMN + 1, :] = pick(upright(cols[s : s + 1, :]), chosen)
            line = pick(row, chosen)
            before = pltpu.roll(line, 1, axis=1)
            first = lax.broadcasted_iota(jnp.int32, line.shape, 1) == 0
            ranks[4 * s + KEEP : 4 * s + KEEP + 1, :] = jnp.where(
                first, 0, jnp.where(line == before, 1, 0)
            )
            upto = pick(jnp.ones_like(row), row <= lane)
            same = pick(jnp.ones_like(row), row == lane)
            ranks[4 * s + LAST : 4 * s + LAST + 1, :] = jnp.where(same > 0, upto, 0)
        return pltpu.make_async_copy(ranks, table, sort_sem)

    tiny[0].wait()
    running[0] = jnp.zeros_like(running[0])
    loads[0].wait()
    loads[1].wait()
    make_pack(feat0, weights1, pack0)
    pl.semaphore_wait(barrier, n + 1)
    halo0 = halo_copies(pack0, ext0, 0)
    for copy in halo0:
        copy.start()
    loads[2].wait()
    make_pack(feat1, weights1, pack1)
    halo1 = halo_copies(pack1, ext1, 1)
    for copy in halo1:
        copy.start()
    for copy in tiny[1:]:
        copy.wait()
    sorting = sort_tiles()
    sorting.start()
    project_own(feat0, weights1, ext0)
    project_own(feat1, weights1, ext1)

    def keep_conv(s):
        def finish(r, total):
            conv[s, r] = jnp.maximum(total, 0.0).astype(jnp.bfloat16)

        return finish

    sorting.wait()
    loads[3].wait()
    for copy in halo0:
        copy.wait_recv()
    convolve(0, ext0, tile0, keep_conv(0))
    for d in offsets:
        even_copy(lax.rem(me + d, n)).start()
    pltpu.make_async_copy(conv.at[0, 2 * me], xbuf.at[0, 2 * me], recv_even.at[me]).start()
    loads[4].wait()
    for copy in halo1:
        copy.wait_recv()
    convolve(1, ext1, tile1, keep_conv(1))
    for d in offsets:
        odd_copy(lax.rem(me + d, n)).start()
    pltpu.make_async_copy(conv.at[1, 2 * me], xbuf.at[0, 2 * me + 1], recv_odd.at[me]).start()
    for d in offsets:
        rest_copy(lax.rem(me + d, n)).start()
    pltpu.make_async_copy(
        conv.at[:, 2 * me + 1], xbuf.at[1, pl.ds(2 * me, 2)], recv_rest.at[me]
    ).start()

    for copy in loads[5:]:
        copy.wait()

    def cell(x, hidden, memory, layer):
        gates = (
            jnp.dot(x, weights[layer, :width], preferred_element_type=jnp.float32)
            + jnp.dot(hidden[...], weights[layer, width:], preferred_element_type=jnp.float32)
            + bias[layer][None, :]
        )
        kept = sigmoid(gates[:, width : 2 * width]) * memory[...]
        new = kept + sigmoid(gates[:, :width]) * jnp.tanh(gates[:, 2 * width : 3 * width])
        memory[...] = new
        result = (sigmoid(gates[:, 3 * width :]) * jnp.tanh(new)).astype(jnp.bfloat16)
        hidden[...] = result
        return result

    backs = (back0, back1)

    def back_copy(half, part, owner):
        return pltpu.make_async_remote_copy(
            src_ref=hbuf.at[half, 2 * owner + part],
            dst_ref=backs[part].at[2 * me + half],
            send_sem=send_back.at[half, part, owner],
            recv_sem=recv_back.at[half, part, me],
            device_id={"snap": owner},
            device_id_type=MESH,
        )

    def give_own(half, part):
        pltpu.make_async_copy(
            hbuf.at[half, 2 * me + part],
            backs[part].at[2 * me + half],
            recv_back.at[half, part, me],
        ).start()

    for half in range(2):
        h0[...] = jnp.zeros_like(h0)
        h1[...] = jnp.zeros_like(h1)
        c0[...] = jnp.zeros_like(c0)
        c1[...] = jnp.zeros_like(c1)

        def step(owner, carry, half=half):
            if half == 0:
                landed(xbuf.at[0, 2 * owner], recv_even.at[owner])
                landed(xbuf.at[0, 2 * owner + 1], recv_odd.at[owner])
            else:
                landed(xbuf.at[1, pl.ds(2 * owner, 2)], recv_rest.at[owner])
            for part in range(2):
                t = 2 * owner + part
                low = cell(xbuf[half, t], h0, c0, 0)
                hbuf[half, t] = cell(low, h1, c1, 1)
            return carry

        lax.fori_loop(0, n, step, 0)
        if half == 0:
            order = [(d, part) for d in offsets for part in range(2)]
        else:
            order = [(d, part) for part in range(2) for d in offsets]
        for d, part in order:
            back_copy(half, part, lax.rem(me + d, n)).start()
        for part in range(2):
            give_own(half, part)

    halos = []
    stores = []
    for part in range(2):
        back, pack, extended = backs[part], (pack2, pack3)[part], (ext2, ext3)[part]
        tile = (tile0, tile1)[part]

        def arrive(source, carry, part=part, back=back):
            for half in range(2):
                landed(back.at[2 * source + half], recv_back.at[half, part, source])
            return carry

        lax.fori_loop(0, n, arrive, 0)
        make_pack(back, weights2, pack)
        copies = halo_copies(pack, extended, 2 + part)
        for copy in copies:
            copy.start()
        project_own(back, weights2, extended)
        for copy in copies:
            copy.wait_recv()
        halos.append(copies)

        def finish(r, total, part=part):
            stage[part, r] = total.astype(jnp.bfloat16)

        convolve(part, extended, tile, finish)
        copy = pltpu.make_async_copy(stage.at[part], out.at[part], store.at[part])
        copy.start()
        stores.append(copy)

    def drain(i, carry):
        peer = lax.rem(me + i, n)
        even_copy(peer).wait_send()
        odd_copy(peer).wait_send()
        rest_copy(peer).wait_send()
        for half in range(2):
            for part in range(2):
                back_copy(half, part, peer).wait_send()
        return carry

    lax.fori_loop(1, n, drain, 0)
    for copies in [halo0, halo1] + halos:
        for copy in copies:
            copy.wait_send()
    for copy in stores:
        copy.wait()


def whole(send_lists, tile_rows, tile_cols, features, tile_vals, w1, w2, lstm_weight, lstm_bias):
    n = lax.axis_size("snap")
    snaps, blocks, _, width = features.shape
    bound = send_lists.shape[0] // 2
    tiles = tile_vals.shape[1]
    total = snaps * n
    hbm = pl.BlockSpec(memory_space=pltpu.HBM)

    def rows(count, dtype=jnp.bfloat16):
        return pltpu.VMEM((count, BS, width), dtype)

    def states(dtype):
        return pltpu.VMEM((BS, width), dtype)

    dma = pltpu.SemaphoreType.DMA
    operands = [
        pltpu.with_memory_space_constraint(x, pltpu.HBM)
        for x in (
            send_lists, tile_rows, tile_cols, features, tile_vals, w1, w2, lstm_weight, lstm_bias
        )
    ]
    return pl.pallas_call(
        functools.partial(whole_kernel, n),
        out_shape=jax.ShapeDtypeStruct(features.shape, jnp.bfloat16),
        in_specs=[hbm] * 9,
        out_specs=pl.BlockSpec(memory_space=pl.ANY),
        scratch_shapes=[
            pltpu.SMEM(send_lists.shape, jnp.int32), pltpu.VMEM(tile_rows.shape, jnp.int32),
            pltpu.VMEM(tile_cols.shape, jnp.int32),
            pltpu.VMEM((8, 128), jnp.int32), pltpu.SMEM((8, 128), jnp.int32),
            rows(blocks), rows(blocks),
            pltpu.VMEM((tiles, BS, BS), jnp.bfloat16), pltpu.VMEM((tiles, BS, BS), jnp.bfloat16),
            rows(blocks + 2 * bound), rows(blocks + 2 * bound),
            rows(blocks + 2 * bound), rows(blocks + 2 * bound),
            rows(2 * bound), rows(2 * bound), rows(2 * bound), rows(2 * bound),
            rows(tiles + 1, jnp.float32),
            pltpu.VMEM((snaps, blocks, BS, width), jnp.bfloat16),
            pltpu.VMEM((2, total, BS, width), jnp.bfloat16),
            pltpu.VMEM((2, total, BS, width), jnp.bfloat16),
            rows(blocks), rows(blocks),
            pltpu.VMEM((snaps, blocks, BS, width), jnp.bfloat16),
            pltpu.VMEM(w1.shape, jnp.bfloat16), pltpu.VMEM(w2.shape, jnp.bfloat16),
            pltpu.VMEM(lstm_weight.shape, jnp.bfloat16), pltpu.VMEM(lstm_bias.shape, jnp.float32),
            states(jnp.bfloat16), states(jnp.float32), states(jnp.bfloat16), states(jnp.float32),
            dma((8,)), dma((2,)), dma((3,)), dma(()), dma((4, 2)), dma((4, 2)),
            dma((n,)), dma((n,)), dma((n,)), dma((n,)), dma((n,)), dma((n,)),
            dma((2, 2, n)), dma((2, 2, n)),
        ],
        compiler_params=pltpu.CompilerParams(
            collective_id=0, has_side_effects=True, vmem_limit_bytes=44 * 2**20
        ),
        cost_estimate=pl.CostEstimate(
            flops=12 << 30, bytes_accessed=11 << 20, transcendentals=42 << 20
        ),
        name="whole",
    )(*operands)


def shards(
    features,
    tile_rows,
    tile_cols,
    tile_vals,
    send_lists,
    conv1_weight,
    conv2_weight,
    lstm_weight,
    lstm_bias,
):
    snapshots, vertices, width = features.shape
    own = features.reshape(snapshots, vertices // BS, BS, width)
    mixed = whole(
        send_lists.T, tile_rows, tile_cols, own, tile_vals,
        conv1_weight, conv2_weight, lstm_weight, lstm_bias,
    )
    return mixed.reshape(snapshots, vertices, width)


def solution(mesh):
    placed = (
        P("snap", "vert", None),
        P("snap", "vert"),
        P("snap", "vert"),
        P("snap", "vert", None, None),
        P(),
        P(),
        P(),
        P(),
        P(),
    )
    return jax.shard_map(
        shards, mesh=mesh, in_specs=placed, out_specs=P("snap", "vert", None), check_vma=False
    )
```

```python
import functools

import jax
import jax.numpy as jnp
from jax import lax
from jax.experimental import pallas as pl
from jax.experimental.pallas import tpu as pltpu
from jax.sharding import PartitionSpec as P

BS = 128
MESH = pl.DeviceIdType.MESH
UNROLL = 32
ORDER, COLUMN, KEEP, LAST, AGAIN = range(5)
BLOCK, PLACE = 10, 11


def sigmoid(x):
    return 0.5 * jnp.tanh(0.5 * x) + 0.5


def whole_kernel(
    n, lists_hbm, rows_hbm, cols_hbm, features, vals, w1, w2, lstm_w, lstm_b, out,
    lists, rows, cols, ranks, table, feat0, feat1, tile0, tile1,
    ext0, ext1, ext2, ext3, pack0, pack1, pack2, pack3, running, conv, xbuf, hbuf, back0, back1, back2, back3,
    weights1, weights2, weights, bias, h0, c0, h1, c1,
    load, tiny_sem, sort_sem, halo_send, halo_recv,
    send_even, send_odd, send_rest, recv_even, recv_odd, recv_rest, send_back, recv_back,
):
    me = lax.axis_index("snap")
    vert = lax.axis_index("vert")
    verts = lax.axis_size("vert")
    lower, higher = lax.rem(vert + verts - 1, verts), lax.rem(vert + 1, verts)
    blocks, width = conv.shape[1], conv.shape[-1]
    bound = lists.shape[0] // 2
    tiles = vals.shape[1]
    offsets = [4, 3, 5, 2, 6, 1, 7] if n == 8 else list(range(1, n))

    tiny = [
        pltpu.make_async_copy(a, b, tiny_sem.at[i])
        for i, (a, b) in enumerate(((lists_hbm, lists), (rows_hbm, rows), (cols_hbm, cols)))
    ]
    for copy in tiny:
        copy.start()
    sources = [w1, features.at[0], features.at[1], vals.at[0], vals.at[1], lstm_w, lstm_b, w2]
    targets = [weights1, feat0, feat1, tile0, tile1, weights, bias, weights2]
    loads = [pltpu.make_async_copy(a, b, load.at[i]) for i, (a, b) in enumerate(zip(sources, targets))]
    for copy in loads:
        copy.start()

    barrier = pltpu.get_barrier_semaphore()
    for d in range(1, n):
        pl.semaphore_signal(
            barrier, inc=1, device_id={"snap": lax.rem(me + d, n)}, device_id_type=MESH
        )
    for side in (lower, higher):
        pl.semaphore_signal(barrier, inc=1, device_id={"vert": side}, device_id_type=MESH)

    def project(block, weight):
        return jnp.dot(block, weight[...], preferred_element_type=jnp.float32).astype(jnp.bfloat16)

    def make_pack(source, weight, pack, place):
        for i in range(2 * bound):
            pack[i] = project(source[place(lists[i, vert])], weight)

    def halo_copies(pack, extended, index):
        down = pltpu.make_async_remote_copy(
            src_ref=pack.at[pl.ds(0, bound)],
            dst_ref=extended.at[pl.ds(bound + blocks, bound)],
            send_sem=halo_send.at[index, 0],
            recv_sem=halo_recv.at[index, 0],
            device_id={"vert": lower},
            device_id_type=MESH,
        )
        up = pltpu.make_async_remote_copy(
            src_ref=pack.at[pl.ds(bound, bound)],
            dst_ref=extended.at[pl.ds(0, bound)],
            send_sem=halo_send.at[index, 1],
            recv_sem=halo_recv.at[index, 1],
            device_id={"vert": higher},
            device_id_type=MESH,
        )
        return (down, up)

    def project_own(source, weight, extended, base):
        def some(g, carry):
            for u in range(4):
                i = 4 * g + u
                extended[base + i] = project(source[i], weight)
            return carry

        lax.fori_loop(0, source.shape[0] // 4, some, 0)

    def convolve(s, kind, extended, tile, block, finish):
        def group(g, carry):
            products = []
            for u in range(UNROLL):
                k = g * UNROLL + u
                products.append(
                    jnp.dot(
                        tile[table[2 * ORDER + s, k]],
                        extended[table[2 * kind + s, k]],
                        preferred_element_type=jnp.float32,
                    )
                )
            total = running[g * UNROLL]
            for u in range(UNROLL):
                k = g * UNROLL + u
                total = total * table[2 * KEEP + s, k].astype(jnp.float32) + products[u]
                running[k + 1] = total
            return carry

        lax.fori_loop(0, tiles // UNROLL, group, 0)

        def some(g, carry):
            for u in range(8):
                r = 8 * g + u
                finish(r, running[table[2 * LAST + s, block(r)]])
            return carry

        lax.fori_loop(0, blocks // 8, some, 0)

    def cross(source, slot, send, recv, peer):
        return pltpu.make_async_remote_copy(
            src_ref=source,
            dst_ref=slot,
            send_sem=send.at[peer],
            recv_sem=recv.at[me],
            device_id={"snap": peer},
            device_id_type=MESH,
        )

    def even_copy(peer):
        return cross(conv.at[0, peer], xbuf.at[0, 2 * me], send_even, recv_even, peer)

    def odd_copy(peer):
        return cross(conv.at[1, peer], xbuf.at[0, 2 * me + 1], send_odd, recv_odd, peer)

    def rest_copy(peer):
        return cross(
            conv.at[:, n + peer], xbuf.at[1, pl.ds(2 * me, 2)], send_rest, recv_rest, peer
        )

    def landed(slot, semaphore):
        pltpu.make_async_copy(slot, slot, semaphore).wait()

    def sort_tiles():
        shape = (tiles, ranks.shape[1])
        lane = lax.broadcasted_iota(jnp.int32, shape, 1)
        sub = lax.broadcasted_iota(jnp.int32, shape, 0)
        square = (tiles, tiles)
        lane_sq = lax.broadcasted_iota(jnp.int32, square, 1)
        sub_sq = lax.broadcasted_iota(jnp.int32, square, 0)

        def upright(line):
            wide = jnp.broadcast_to(line, square)
            return jnp.sum(jnp.where(lane_sq == sub_sq, wide, 0), axis=1, keepdims=True)

        def pick(column, chosen):
            return jnp.sum(jnp.where(chosen, column, 0), axis=0, keepdims=True)

        few = (blocks, blocks)
        lane_few = lax.broadcasted_iota(jnp.int32, few, 1)
        sub_few = lax.broadcasted_iota(jnp.int32, few, 0)
        lane_line = lax.broadcasted_iota(jnp.int32, (1, ranks.shape[1]), 1)

        def line_at(kind, value):
            ranks[kind : kind + 1, :] = value

        def unlisted(index):
            value = jnp.ones_like(index)
            for i in range(2 * bound):
                value = jnp.where(index == lists[i, vert], 0, value)
            return value * blocks + index

        key_up = unlisted(lax.broadcasted_iota(jnp.int32, (blocks, ranks.shape[1]), 0))
        key_line = unlisted(lane_line)
        place_line = jnp.sum(jnp.where(key_up < key_line, 1, 0), axis=0, keepdims=True)
        line_at(PLACE, place_line)
        smaller = jnp.where(unlisted(lane_few) < unlisted(sub_few), 1, 0)
        place = jnp.sum(smaller, axis=1, keepdims=True)
        wide = (blocks, ranks.shape[1])
        line_at(
            BLOCK,
            pick(
                lax.broadcasted_iota(jnp.int32, wide, 0),
                place == lax.broadcasted_iota(jnp.int32, wide, 1),
            ),
        )
        for s in range(rows.shape[0]):
            row_line = rows[s : s + 1, :]
            row = upright(row_line)
            col = upright(cols[s : s + 1, :])
            key = jnp.broadcast_to(row_line, square) * tiles + lane_sq
            smaller = jnp.where(key < row * tiles + sub_sq, 1, 0)
            rank = jnp.sum(smaller, axis=1, keepdims=True)
            chosen = rank == lane
            line_at(2 * ORDER + s, pick(sub, chosen))
            line_at(2 * COLUMN + s, pick(col, chosen))
            moved = jnp.where(lane == col - bound, place_line, 0)
            moved = jnp.sum(moved, axis=1, keepdims=True) + bound
            inner = jnp.where(col >= bound, jnp.where(col < bound + blocks, 1, 0), 0)
            line_at(2 * AGAIN + s, pick(jnp.where(inner == 1, moved, col), chosen))
            line = pick(row, chosen)
            same = jnp.where(line == pltpu.roll(line, 1, axis=1), 1, 0)
            line_at(2 * KEEP + s, jnp.where(lane_line == 0, 0, same))
            upto = pick(jnp.ones_like(row), row <= lane)
            found = pick(jnp.ones_like(row), row == lane)
            line_at(2 * LAST + s, jnp.where(found > 0, upto, 0))
        return pltpu.make_async_copy(ranks, table, sort_sem)

    tiny[0].wait()
    running[0] = jnp.zeros_like(running[0])
    loads[0].wait()
    loads[1].wait()
    make_pack(feat0, weights1, pack0, lambda b: b)
    pl.semaphore_wait(barrier, n + 1)
    halo0 = halo_copies(pack0, ext0, 0)
    for copy in halo0:
        copy.start()
    loads[2].wait()
    make_pack(feat1, weights1, pack1, lambda b: b)
    halo1 = halo_copies(pack1, ext1, 1)
    for copy in halo1:
        copy.start()
    for copy in tiny[1:]:
        copy.wait()
    sorting = sort_tiles()
    sorting.start()
    project_own(feat0, weights1, ext0, bound)
    project_own(feat1, weights1, ext1, bound)

    def keep_conv(s):
        def finish(r, total):
            conv[s, r] = jnp.maximum(total, 0.0).astype(jnp.bfloat16)

        return finish

    sorting.wait()
    loads[3].wait()
    for copy in halo0:
        copy.wait_recv()
    convolve(0, COLUMN, ext0, tile0, lambda p: table[BLOCK, p], keep_conv(0))
    for d in offsets:
        even_copy(lax.rem(me + d, n)).start()
    pltpu.make_async_copy(conv.at[0, me], xbuf.at[0, 2 * me], recv_even.at[me]).start()
    loads[4].wait()
    for copy in halo1:
        copy.wait_recv()
    convolve(1, COLUMN, ext1, tile1, lambda p: table[BLOCK, p], keep_conv(1))
    for d in offsets:
        odd_copy(lax.rem(me + d, n)).start()
    pltpu.make_async_copy(conv.at[1, me], xbuf.at[0, 2 * me + 1], recv_odd.at[me]).start()
    for d in offsets:
        rest_copy(lax.rem(me + d, n)).start()
    pltpu.make_async_copy(
        conv.at[:, n + me], xbuf.at[1, pl.ds(2 * me, 2)], recv_rest.at[me]
    ).start()

    for copy in loads[5:]:
        copy.wait()

    def cell(x, hidden, memory, layer):
        gates = (
            jnp.dot(x, weights[layer, :width], preferred_element_type=jnp.float32)
            + jnp.dot(hidden[...], weights[layer, width:], preferred_element_type=jnp.float32)
            + bias[layer][None, :]
        )
        kept = sigmoid(gates[:, width : 2 * width]) * memory[...]
        new = kept + sigmoid(gates[:, :width]) * jnp.tanh(gates[:, 2 * width : 3 * width])
        memory[...] = new
        result = (sigmoid(gates[:, 3 * width :]) * jnp.tanh(new)).astype(jnp.bfloat16)
        hidden[...] = result
        return result

    backs = ((back0, back1), (back2, back3))

    def back_copy(half, part, owner):
        return pltpu.make_async_remote_copy(
            src_ref=hbuf.at[half, 2 * owner + part],
            dst_ref=backs[part][half].at[me],
            send_sem=send_back.at[half, part, owner],
            recv_sem=recv_back.at[half, part, me],
            device_id={"snap": owner},
            device_id_type=MESH,
        )

    def give_own(half, part):
        pltpu.make_async_copy(
            hbuf.at[half, 2 * me + part],
            backs[part][half].at[me],
            recv_back.at[half, part, me],
        ).start()

    for half in range(2):
        h0[...] = jnp.zeros_like(h0)
        h1[...] = jnp.zeros_like(h1)
        c0[...] = jnp.zeros_like(c0)
        c1[...] = jnp.zeros_like(c1)

        def step(owner, carry, half=half):
            if half == 0:
                landed(xbuf.at[0, 2 * owner], recv_even.at[owner])
                landed(xbuf.at[0, 2 * owner + 1], recv_odd.at[owner])
            else:
                landed(xbuf.at[1, pl.ds(2 * owner, 2)], recv_rest.at[owner])
            for part in range(2):
                t = 2 * owner + part
                low = cell(xbuf[half, t], h0, c0, 0)
                hbuf[half, t] = cell(low, h1, c1, 1)
            return carry

        lax.fori_loop(0, n, step, 0)
        if half == 0:
            order = [(d, part) for d in offsets for part in range(2)]
        else:
            order = [(d, part) for part in range(2) for d in offsets]
        for d, part in order:
            back_copy(half, part, lax.rem(me + d, n)).start()
        for part in range(2):
            give_own(half, part)

    def arrive(part, half):
        def one(source, carry):
            landed(backs[part][half].at[source], recv_back.at[half, part, source])
            return carry

        lax.fori_loop(0, n, one, 0)

    packs, wides, grids = (pack2, pack3), (ext2, ext3), (tile0, tile1)
    halos = []
    for part in range(2):
        arrive(part, 0)
        make_pack(backs[part][0], weights2, packs[part], lambda b: table[PLACE, b])
        copies = halo_copies(packs[part], wides[part], 2 + part)
        for copy in copies:
            copy.start()
        halos.append(copies)
    for part in range(2):
        project_own(backs[part][0], weights2, wides[part], bound)
    for part in range(2):
        arrive(part, 1)
        project_own(backs[part][1], weights2, wides[part], bound + n)
        for copy in halos[part]:
            copy.wait_recv()

        def finish(r, total, part=part):
            out[part, r] = total.astype(jnp.bfloat16)

        convolve(part, AGAIN, wides[part], grids[part], lambda r: r, finish)

    def drain(i, carry):
        peer = lax.rem(me + i, n)
        even_copy(peer).wait_send()
        odd_copy(peer).wait_send()
        rest_copy(peer).wait_send()
        for half in range(2):
            for part in range(2):
                back_copy(half, part, peer).wait_send()
        return carry

    lax.fori_loop(1, n, drain, 0)
    for copies in [halo0, halo1] + halos:
        for copy in copies:
            copy.wait_send()


def whole(send_lists, tile_rows, tile_cols, features, tile_vals, w1, w2, lstm_weight, lstm_bias):
    n = lax.axis_size("snap")
    snaps, blocks, _, width = features.shape
    bound = send_lists.shape[0] // 2
    tiles = tile_vals.shape[1]
    total = snaps * n
    hbm = pl.BlockSpec(memory_space=pltpu.HBM)

    def rows(count, dtype=jnp.bfloat16):
        return pltpu.VMEM((count, BS, width), dtype)

    def states(dtype):
        return pltpu.VMEM((BS, width), dtype)

    dma = pltpu.SemaphoreType.DMA
    operands = [
        pltpu.with_memory_space_constraint(x, pltpu.HBM)
        for x in (
            send_lists, tile_rows, tile_cols, features, tile_vals, w1, w2, lstm_weight, lstm_bias
        )
    ]
    return pl.pallas_call(
        functools.partial(whole_kernel, n),
        out_shape=jax.ShapeDtypeStruct(features.shape, jnp.bfloat16),
        in_specs=[hbm] * 9,
        out_specs=pl.BlockSpec(memory_space=pltpu.VMEM),
        scratch_shapes=[
            pltpu.SMEM(send_lists.shape, jnp.int32), pltpu.VMEM(tile_rows.shape, jnp.int32),
            pltpu.VMEM(tile_cols.shape, jnp.int32),
            pltpu.VMEM((16, 128), jnp.int32), pltpu.SMEM((16, 128), jnp.int32),
            rows(blocks), rows(blocks),
            pltpu.VMEM((tiles, BS, BS), jnp.bfloat16), pltpu.VMEM((tiles, BS, BS), jnp.bfloat16),
            rows(blocks + 2 * bound), rows(blocks + 2 * bound),
            rows(blocks + 2 * bound), rows(blocks + 2 * bound),
            rows(2 * bound), rows(2 * bound), rows(2 * bound), rows(2 * bound),
            rows(tiles + 1, jnp.float32),
            pltpu.VMEM((snaps, blocks, BS, width), jnp.bfloat16),
            pltpu.VMEM((2, total, BS, width), jnp.bfloat16),
            pltpu.VMEM((2, total, BS, width), jnp.bfloat16),
            rows(n), rows(n), rows(n), rows(n),
            pltpu.VMEM(w1.shape, jnp.bfloat16), pltpu.VMEM(w2.shape, jnp.bfloat16),
            pltpu.VMEM(lstm_weight.shape, jnp.bfloat16), pltpu.VMEM(lstm_bias.shape, jnp.float32),
            states(jnp.bfloat16), states(jnp.float32), states(jnp.bfloat16), states(jnp.float32),
            dma((8,)), dma((3,)), dma(()), dma((4, 2)), dma((4, 2)),
            dma((n,)), dma((n,)), dma((n,)), dma((n,)), dma((n,)), dma((n,)),
            dma((2, 2, n)), dma((2, 2, n)),
        ],
        compiler_params=pltpu.CompilerParams(
            collective_id=0, has_side_effects=True, vmem_limit_bytes=44 * 2**20
        ),
        cost_estimate=pl.CostEstimate(
            flops=12 << 30, bytes_accessed=11 << 20, transcendentals=42 << 20
        ),
        name="whole",
    )(*operands)


def shards(
    features,
    tile_rows,
    tile_cols,
    tile_vals,
    send_lists,
    conv1_weight,
    conv2_weight,
    lstm_weight,
    lstm_bias,
):
    snapshots, vertices, width = features.shape
    own = features.reshape(snapshots, vertices // BS, BS, width)
    mixed = whole(
        send_lists.T, tile_rows, tile_cols, own, tile_vals,
        conv1_weight, conv2_weight, lstm_weight, lstm_bias,
    )
    return mixed.reshape(snapshots, vertices, width)


def solution(mesh):
    placed = (
        P("snap", "vert", None),
        P("snap", "vert"),
        P("snap", "vert"),
        P("snap", "vert", None, None),
        P(),
        P(),
        P(),
        P(),
        P(),
    )
    return jax.shard_map(
        shards, mesh=mesh, in_specs=placed, out_specs=P("snap", "vert", None), check_vma=False
    )
```

```python
import functools

import jax
import jax.numpy as jnp
from jax import lax
from jax.experimental import pallas as pl
from jax.experimental.pallas import tpu as pltpu
from jax.sharding import PartitionSpec as P

BS = 128
MESH = pl.DeviceIdType.MESH
UNROLL = 20
KEEP, LAST, ORDER, COLUMN, AGAIN = 0, 1, 2, 4, 6
BLOCK, PLACE = 16, 17


def sigmoid(x):
    return 0.5 * jnp.tanh(0.5 * x) + 0.5


def whole_kernel(
    n, lists_hbm, rows_hbm, cols_hbm, features, vals, w1, w2, lstm_w, lstm_b, out,
    lists, rows, cols, ranks, table, feat0, feat1, tile0, tile1,
    ext0, ext1, ext2, ext3, pack0, pack1, pack2, pack3, running, conv, xbuf, hbuf, back0, back1, back2, back3,
    weights1, weights2, weights, bias, h0, c0, h1, c1,
    load, tiny_sem, sort_sem, halo_send, halo_recv,
    send_even, send_odd, send_rest, recv_even, recv_odd, recv_rest, send_back, recv_back,
):
    me = lax.axis_index("snap")
    vert = lax.axis_index("vert")
    verts = lax.axis_size("vert")
    lower, higher = lax.rem(vert + verts - 1, verts), lax.rem(vert + 1, verts)
    blocks, width = conv.shape[1], conv.shape[-1]
    bound = lists.shape[0] // 2
    tiles = vals.shape[1]
    pairs = (tiles + blocks) // 2
    offsets = [4, 3, 5, 2, 6, 1, 7] if n == 8 else list(range(1, n))

    tiny = [
        pltpu.make_async_copy(a, b, tiny_sem.at[i])
        for i, (a, b) in enumerate(((lists_hbm, lists), (rows_hbm, rows), (cols_hbm, cols)))
    ]
    sources = [w1, features.at[0], features.at[1], vals.at[0], vals.at[1], lstm_w, lstm_b, w2]
    targets = [
        weights1, feat0, feat1, tile0.at[pl.ds(0, tiles)], tile1.at[pl.ds(0, tiles)],
        weights, bias, weights2,
    ]
    loads = [pltpu.make_async_copy(a, b, load.at[i]) for i, (a, b) in enumerate(zip(sources, targets))]
    barrier = pltpu.get_barrier_semaphore()
    for side in (lower, higher):
        pl.semaphore_signal(barrier, inc=1, device_id={"vert": side}, device_id_type=MESH)
    for d in range(1, n):
        pl.semaphore_signal(
            barrier, inc=1, device_id={"snap": lax.rem(me + d, n)}, device_id_type=MESH
        )
    for copy in [tiny[0]] + loads[:2]:
        copy.start()

    def project(block, weight):
        return jnp.dot(block, weight[...], preferred_element_type=jnp.float32).astype(jnp.bfloat16)

    def make_pack(source, weight, pack, place):
        for i in range(2 * bound):
            pack[i] = project(source[place(lists[i, vert])], weight)

    def halo_copies(pack, extended, index):
        down = pltpu.make_async_remote_copy(
            src_ref=pack.at[pl.ds(0, bound)],
            dst_ref=extended.at[pl.ds(bound + blocks, bound)],
            send_sem=halo_send.at[index, 0],
            recv_sem=halo_recv.at[index, 0],
            device_id={"vert": lower},
            device_id_type=MESH,
        )
        up = pltpu.make_async_remote_copy(
            src_ref=pack.at[pl.ds(bound, bound)],
            dst_ref=extended.at[pl.ds(0, bound)],
            send_sem=halo_send.at[index, 1],
            recv_sem=halo_recv.at[index, 1],
            device_id={"vert": higher},
            device_id_type=MESH,
        )
        return (down, up)

    def project_own(source, weight, extended, base):
        def some(g, carry):
            for u in range(4):
                i = 4 * g + u
                extended[base + i] = project(source[i], weight)
            return carry

        lax.fori_loop(0, source.shape[0] // 4, some, 0)

    def convolve(s, kind, extended, tile, block, finish, between=None):
        def group(g, carry):
            products = []
            for u in range(UNROLL):
                q = g * UNROLL + u
                left = [tile[table[2 * (ORDER + side) + s, q]] for side in range(2)]
                right = [extended[table[2 * (kind + side) + s, q]] for side in range(2)]
                products.append(
                    jnp.dot(
                        jnp.concatenate(left, axis=1),
                        jnp.concatenate(right, axis=0),
                        preferred_element_type=jnp.float32,
                    )
                )
            total = running[g * UNROLL]
            for u in range(UNROLL):
                q = g * UNROLL + u
                total = total * table[2 * KEEP + s, q].astype(jnp.float32) + products[u]
                running[q + 1] = total
            return carry

        lax.fori_loop(0, pairs // UNROLL, group, 0)
        for half in range(2):
            for u in range(n):
                r = half * n + u
                finish(r, running[table[2 * LAST + s, block(r)]])
            if between is not None and half == 0:
                between()

    def cross(source, slot, send, recv, peer):
        return pltpu.make_async_remote_copy(
            src_ref=source,
            dst_ref=slot,
            send_sem=send.at[peer],
            recv_sem=recv.at[me],
            device_id={"snap": peer},
            device_id_type=MESH,
        )

    def even_copy(peer):
        return cross(conv.at[0, peer], xbuf.at[0, 2 * me], send_even, recv_even, peer)

    def odd_copy(peer):
        return cross(conv.at[1, peer], xbuf.at[0, 2 * me + 1], send_odd, recv_odd, peer)

    def rest_copy(peer):
        return cross(
            conv.at[:, n + peer], xbuf.at[1, pl.ds(2 * me, 2)], send_rest, recv_rest, peer
        )

    def landed(slot, semaphore):
        pltpu.make_async_copy(slot, slot, semaphore).wait()

    def sort_tiles():
        shape = (tiles, ranks.shape[1])
        lane = lax.broadcasted_iota(jnp.int32, shape, 1)
        sub = lax.broadcasted_iota(jnp.int32, shape, 0)
        square = (tiles, tiles)
        lane_sq = lax.broadcasted_iota(jnp.int32, square, 1)
        sub_sq = lax.broadcasted_iota(jnp.int32, square, 0)

        def upright(line):
            wide = jnp.broadcast_to(line, square)
            return jnp.sum(jnp.where(lane_sq == sub_sq, wide, 0), axis=1, keepdims=True)

        def pick(column, chosen):
            return jnp.sum(jnp.where(chosen, column, 0), axis=0, keepdims=True)

        few = (blocks, blocks)
        lane_few = lax.broadcasted_iota(jnp.int32, few, 1)
        sub_few = lax.broadcasted_iota(jnp.int32, few, 0)
        lane_line = lax.broadcasted_iota(jnp.int32, (1, ranks.shape[1]), 1)

        def line_at(kind, value):
            ranks[kind : kind + 1, :] = value

        def unlisted(index):
            value = jnp.ones_like(index)
            for i in range(2 * bound):
                value = jnp.where(index == lists[i, vert], 0, value)
            return value * blocks + index

        key_up = unlisted(lax.broadcasted_iota(jnp.int32, (blocks, ranks.shape[1]), 0))
        key_line = unlisted(lane_line)
        place_line = jnp.sum(jnp.where(key_up < key_line, 1, 0), axis=0, keepdims=True)
        line_at(PLACE, place_line)
        smaller = jnp.where(unlisted(lane_few) < unlisted(sub_few), 1, 0)
        place = jnp.sum(smaller, axis=1, keepdims=True)
        wide = (blocks, ranks.shape[1])
        line_at(
            BLOCK,
            pick(
                lax.broadcasted_iota(jnp.int32, wide, 0),
                place == lax.broadcasted_iota(jnp.int32, wide, 1),
            ),
        )
        for s in range(rows.shape[0]):
            row_line = rows[s : s + 1, :]
            row = upright(row_line)
            col = upright(cols[s : s + 1, :])
            earlier = jnp.where(lane_sq < sub_sq, 1, 0)
            alike = jnp.where(jnp.broadcast_to(row_line, square) == row, earlier, 0)
            within = jnp.sum(alike, axis=1, keepdims=True)
            found = pick(jnp.ones_like(row), row == lane)
            padded = found + (found & 1)
            base = jnp.sum(jnp.where(lane < row, padded, 0), axis=1, keepdims=True)
            spot = base + within
            moved = jnp.where(lane == col - bound, place_line, 0)
            moved = jnp.sum(moved, axis=1, keepdims=True) + bound
            inner = jnp.where(col >= bound, jnp.where(col < bound + blocks, 1, 0), 0)
            again = jnp.where(inner == 1, moved, col)
            for side in range(2):
                chosen = spot == 2 * lane + side
                count = pick(jnp.ones_like(row), chosen)
                line_at(2 * (ORDER + side) + s, jnp.where(count > 0, pick(sub, chosen), tiles))
                line_at(2 * (COLUMN + side) + s, pick(col, chosen))
                line_at(2 * (AGAIN + side) + s, pick(again, chosen))
            line = pick(row, spot == 2 * lane)
            same = jnp.where(line == pltpu.roll(line, 1, axis=1), 1, 0)
            line_at(2 * KEEP + s, jnp.where(lane_line == 0, 0, same))
            wide_pad = jnp.broadcast_to(padded, wide)
            wide_lane = lax.broadcasted_iota(jnp.int32, wide, 1)
            wide_sub = lax.broadcasted_iota(jnp.int32, wide, 0)
            pad = jnp.sum(jnp.where(wide_lane == wide_sub, wide_pad, 0), axis=1, keepdims=True)
            upto = jnp.sum(jnp.where(wide_sub <= wide_lane, pad, 0), axis=0, keepdims=True)
            line_at(2 * LAST + s, jnp.where(found > 0, upto >> 1, 0))
        return pltpu.make_async_copy(ranks, table, sort_sem)

    tiny[0].wait()
    running[0] = jnp.zeros_like(running[0])
    for tile in (tile0, tile1):
        tile[tiles] = jnp.zeros_like(tile[tiles])
    loads[0].wait()
    loads[1].wait()
    for copy in loads[2:] + tiny[1:]:
        copy.start()
    make_pack(feat0, weights1, pack0, lambda b: b)
    pl.semaphore_wait(barrier, n + 1)
    halo0 = halo_copies(pack0, ext0, 0)
    for copy in halo0:
        copy.start()
    loads[2].wait()
    make_pack(feat1, weights1, pack1, lambda b: b)
    halo1 = halo_copies(pack1, ext1, 1)
    for copy in halo1:
        copy.start()
    for copy in tiny[1:]:
        copy.wait()
    sorting = sort_tiles()
    sorting.start()
    project_own(feat0, weights1, ext0, bound)
    project_own(feat1, weights1, ext1, bound)

    def keep_conv(s):
        def finish(r, total):
            conv[s, r] = jnp.maximum(total, 0.0).astype(jnp.bfloat16)

        return finish

    sorting.wait()
    loads[3].wait()
    for copy in halo0:
        copy.wait_recv()

    def send_evens():
        for d in offsets:
            even_copy(lax.rem(me + d, n)).start()
        pltpu.make_async_copy(conv.at[0, me], xbuf.at[0, 2 * me], recv_even.at[me]).start()

    convolve(0, COLUMN, ext0, tile0, lambda p: table[BLOCK, p], keep_conv(0), send_evens)
    loads[4].wait()
    for copy in halo1:
        copy.wait_recv()
    convolve(1, COLUMN, ext1, tile1, lambda p: table[BLOCK, p], keep_conv(1))
    for d in offsets:
        odd_copy(lax.rem(me + d, n)).start()
    pltpu.make_async_copy(conv.at[1, me], xbuf.at[0, 2 * me + 1], recv_odd.at[me]).start()
    for d in offsets:
        rest_copy(lax.rem(me + d, n)).start()
    pltpu.make_async_copy(
        conv.at[:, n + me], xbuf.at[1, pl.ds(2 * me, 2)], recv_rest.at[me]
    ).start()

    for copy in loads[5:]:
        copy.wait()

    def cell(x, hidden, memory, layer):
        gates = (
            jnp.dot(x, weights[layer, :width], preferred_element_type=jnp.float32)
            + jnp.dot(hidden[...], weights[layer, width:], preferred_element_type=jnp.float32)
            + bias[layer][None, :]
        )
        kept = sigmoid(gates[:, width : 2 * width]) * memory[...]
        new = kept + sigmoid(gates[:, :width]) * jnp.tanh(gates[:, 2 * width : 3 * width])
        memory[...] = new
        result = (sigmoid(gates[:, 3 * width :]) * jnp.tanh(new)).astype(jnp.bfloat16)
        hidden[...] = result
        return result

    backs = ((back0, back1), (back2, back3))

    def back_copy(half, part, owner):
        return pltpu.make_async_remote_copy(
            src_ref=hbuf.at[half, 2 * owner + part],
            dst_ref=backs[part][half].at[me],
            send_sem=send_back.at[half, part, owner],
            recv_sem=recv_back.at[half, part, me],
            device_id={"snap": owner},
            device_id_type=MESH,
        )

    def give_own(half, part):
        pltpu.make_async_copy(
            hbuf.at[half, 2 * me + part],
            backs[part][half].at[me],
            recv_back.at[half, part, me],
        ).start()

    for half in range(2):
        h0[...] = jnp.zeros_like(h0)
        h1[...] = jnp.zeros_like(h1)
        c0[...] = jnp.zeros_like(c0)
        c1[...] = jnp.zeros_like(c1)

        def step(owner, carry, half=half):
            if half == 0:
                landed(xbuf.at[0, 2 * owner], recv_even.at[owner])
                landed(xbuf.at[0, 2 * owner + 1], recv_odd.at[owner])
            else:
                landed(xbuf.at[1, pl.ds(2 * owner, 2)], recv_rest.at[owner])
            for part in range(2):
                t = 2 * owner + part
                low = cell(xbuf[half, t], h0, c0, 0)
                hbuf[half, t] = cell(low, h1, c1, 1)
            return carry

        lax.fori_loop(0, n, step, 0)
        if half == 0:
            order = [(d, part) for d in offsets for part in range(2)]
        else:
            order = [(d, part) for part in range(2) for d in offsets]
        for d, part in order:
            back_copy(half, part, lax.rem(me + d, n)).start()
        for part in range(2):
            give_own(half, part)

    def arrive(part, half):
        def one(source, carry):
            landed(backs[part][half].at[source], recv_back.at[half, part, source])
            return carry

        lax.fori_loop(0, n, one, 0)

    packs, wides, grids = (pack2, pack3), (ext2, ext3), (tile0, tile1)
    halos = []
    for part in range(2):
        arrive(part, 0)
        make_pack(backs[part][0], weights2, packs[part], lambda b: table[PLACE, b])
        copies = halo_copies(packs[part], wides[part], 2 + part)
        for copy in copies:
            copy.start()
        halos.append(copies)
    for part in range(2):
        project_own(backs[part][0], weights2, wides[part], bound)
    for part in range(2):
        arrive(part, 1)
        project_own(backs[part][1], weights2, wides[part], bound + n)
        for copy in halos[part]:
            copy.wait_recv()

        def finish(r, total, part=part):
            out[part, r] = total.astype(jnp.bfloat16)

        convolve(part, AGAIN, wides[part], grids[part], lambda r: r, finish)

    def drain(i, carry):
        peer = lax.rem(me + i, n)
        even_copy(peer).wait_send()
        odd_copy(peer).wait_send()
        rest_copy(peer).wait_send()
        for half in range(2):
            for part in range(2):
                back_copy(half, part, peer).wait_send()
        return carry

    lax.fori_loop(1, n, drain, 0)
    for copies in [halo0, halo1] + halos:
        for copy in copies:
            copy.wait_send()


def whole(send_lists, tile_rows, tile_cols, features, tile_vals, w1, w2, lstm_weight, lstm_bias):
    n = lax.axis_size("snap")
    snaps, blocks, _, width = features.shape
    bound = send_lists.shape[0] // 2
    tiles = tile_vals.shape[1]
    total = snaps * n
    hbm = pl.BlockSpec(memory_space=pltpu.HBM)

    def rows(count, dtype=jnp.bfloat16):
        return pltpu.VMEM((count, BS, width), dtype)

    def states(dtype):
        return pltpu.VMEM((BS, width), dtype)

    dma = pltpu.SemaphoreType.DMA
    operands = [
        pltpu.with_memory_space_constraint(x, pltpu.HBM)
        for x in (
            send_lists, tile_rows, tile_cols, features, tile_vals, w1, w2, lstm_weight, lstm_bias
        )
    ]
    return pl.pallas_call(
        functools.partial(whole_kernel, n),
        out_shape=jax.ShapeDtypeStruct(features.shape, jnp.bfloat16),
        in_specs=[hbm] * 9,
        out_specs=pl.BlockSpec(memory_space=pltpu.VMEM),
        scratch_shapes=[
            pltpu.SMEM(send_lists.shape, jnp.int32), pltpu.VMEM(tile_rows.shape, jnp.int32),
            pltpu.VMEM(tile_cols.shape, jnp.int32),
            pltpu.VMEM((24, 128), jnp.int32), pltpu.SMEM((24, 128), jnp.int32),
            rows(blocks), rows(blocks),
            pltpu.VMEM((tiles + 1, BS, BS), jnp.bfloat16),
            pltpu.VMEM((tiles + 1, BS, BS), jnp.bfloat16),
            rows(blocks + 2 * bound), rows(blocks + 2 * bound),
            rows(blocks + 2 * bound), rows(blocks + 2 * bound),
            rows(2 * bound), rows(2 * bound), rows(2 * bound), rows(2 * bound),
            rows((tiles + blocks) // 2 + 1, jnp.float32),
            pltpu.VMEM((snaps, blocks, BS, width), jnp.bfloat16),
            pltpu.VMEM((2, total, BS, width), jnp.bfloat16),
            pltpu.VMEM((2, total, BS, width), jnp.bfloat16),
            rows(n), rows(n), rows(n), rows(n),
            pltpu.VMEM(w1.shape, jnp.bfloat16), pltpu.VMEM(w2.shape, jnp.bfloat16),
            pltpu.VMEM(lstm_weight.shape, jnp.bfloat16), pltpu.VMEM(lstm_bias.shape, jnp.float32),
            states(jnp.bfloat16), states(jnp.float32), states(jnp.bfloat16), states(jnp.float32),
            dma((8,)), dma((3,)), dma(()), dma((4, 2)), dma((4, 2)),
            dma((n,)), dma((n,)), dma((n,)), dma((n,)), dma((n,)), dma((n,)),
            dma((2, 2, n)), dma((2, 2, n)),
        ],
        compiler_params=pltpu.CompilerParams(
            collective_id=0, has_side_effects=True, vmem_limit_bytes=44 * 2**20
        ),
        cost_estimate=pl.CostEstimate(
            flops=12 << 30, bytes_accessed=11 << 20, transcendentals=42 << 20
        ),
        name="whole",
    )(*operands)


def shards(
    features,
    tile_rows,
    tile_cols,
    tile_vals,
    send_lists,
    conv1_weight,
    conv2_weight,
    lstm_weight,
    lstm_bias,
):
    snapshots, vertices, width = features.shape
    own = features.reshape(snapshots, vertices // BS, BS, width)
    mixed = whole(
        send_lists.T, tile_rows, tile_cols, own, tile_vals,
        conv1_weight, conv2_weight, lstm_weight, lstm_bias,
    )
    return mixed.reshape(snapshots, vertices, width)


def solution(mesh):
    placed = (
        P("snap", "vert", None),
        P("snap", "vert"),
        P("snap", "vert"),
        P("snap", "vert", None, None),
        P(),
        P(),
        P(),
        P(),
        P(),
    )
    return jax.shard_map(
        shards, mesh=mesh, in_specs=placed, out_specs=P("snap", "vert", None), check_vma=False
    )
```

```python
import functools

import jax
import jax.numpy as jnp
from jax import lax
from jax.experimental import pallas as pl
from jax.experimental.pallas import tpu as pltpu
from jax.sharding import PartitionSpec as P

BS = 128
MESH = pl.DeviceIdType.MESH
UNROLL = 20
KEEP, LAST, ORDER, COLUMN, AGAIN = 0, 1, 2, 4, 6
BLOCK, PLACE = 16, 17


def sigmoid(x):
    return 0.5 * jnp.tanh(0.5 * x) + 0.5


def whole_kernel(
    n, lists_hbm, rows_hbm, cols_hbm, features, vals, w1, w2, lstm_w, lstm_b, out,
    lists, rows, cols, ranks, table, feat0, feat1, tile0, tile1,
    ext0, ext1, ext2, ext3, pack0, pack1, pack2, pack3, running, conv, xbuf, hbuf, early, late0, late1,
    weights1, weights2, weights, bias, h0, c0, h1, c1,
    load, tiny_sem, sort_sem, halo_send, halo_recv,
    send_even, send_odd, send_rest, recv_even, recv_odd, recv_rest, send_early, recv_early, send_late, recv_late,
):
    me = lax.axis_index("snap")
    vert = lax.axis_index("vert")
    verts = lax.axis_size("vert")
    lower, higher = lax.rem(vert + verts - 1, verts), lax.rem(vert + 1, verts)
    blocks, width = conv.shape[1], conv.shape[-1]
    bound = lists.shape[0] // 2
    tiles = vals.shape[1]
    pairs = (tiles + blocks) // 2
    offsets = [4, 3, 5, 2, 6, 1, 7] if n == 8 else list(range(1, n))

    tiny = [
        pltpu.make_async_copy(a, b, tiny_sem.at[i])
        for i, (a, b) in enumerate(((lists_hbm, lists), (rows_hbm, rows), (cols_hbm, cols)))
    ]
    sources = [w1, features.at[0], features.at[1], vals.at[0], vals.at[1], lstm_w, lstm_b, w2]
    targets = [
        weights1, feat0, feat1, tile0.at[pl.ds(0, tiles)], tile1.at[pl.ds(0, tiles)],
        weights, bias, weights2,
    ]
    loads = [pltpu.make_async_copy(a, b, load.at[i]) for i, (a, b) in enumerate(zip(sources, targets))]
    barrier = pltpu.get_barrier_semaphore()
    for side in (lower, higher):
        pl.semaphore_signal(barrier, inc=1, device_id={"vert": side}, device_id_type=MESH)
    for d in range(1, n):
        pl.semaphore_signal(
            barrier, inc=1, device_id={"snap": lax.rem(me + d, n)}, device_id_type=MESH
        )
    for copy in [tiny[0]] + loads[:2]:
        copy.start()

    def project(block, weight):
        return jnp.dot(block, weight[...], preferred_element_type=jnp.float32).astype(jnp.bfloat16)

    def make_pack(source, weight, pack):
        for i in range(2 * bound):
            pack[i] = project(source(lists[i, vert]), weight)

    def halo_copies(pack, extended, index):
        down = pltpu.make_async_remote_copy(
            src_ref=pack.at[pl.ds(0, bound)],
            dst_ref=extended.at[pl.ds(bound + blocks, bound)],
            send_sem=halo_send.at[index, 0],
            recv_sem=halo_recv.at[index, 0],
            device_id={"vert": lower},
            device_id_type=MESH,
        )
        up = pltpu.make_async_remote_copy(
            src_ref=pack.at[pl.ds(bound, bound)],
            dst_ref=extended.at[pl.ds(0, bound)],
            send_sem=halo_send.at[index, 1],
            recv_sem=halo_recv.at[index, 1],
            device_id={"vert": higher},
            device_id_type=MESH,
        )
        return (down, up)

    def project_own(source, count, weight, extended, base):
        def some(g, carry):
            for u in range(4):
                i = 4 * g + u
                extended[base + i] = project(source(i), weight)
            return carry

        lax.fori_loop(0, count // 4, some, 0)

    def convolve(s, kind, extended, tile, block, finish, between=None):
        def group(g, carry):
            products = []
            for u in range(UNROLL):
                q = g * UNROLL + u
                left = [tile[table[2 * (ORDER + side) + s, q]] for side in range(2)]
                right = [extended[table[2 * (kind + side) + s, q]] for side in range(2)]
                products.append(
                    jnp.dot(
                        jnp.concatenate(left, axis=1),
                        jnp.concatenate(right, axis=0),
                        preferred_element_type=jnp.float32,
                    )
                )
            total = running[g * UNROLL]
            for u in range(UNROLL):
                q = g * UNROLL + u
                total = total * table[2 * KEEP + s, q].astype(jnp.float32) + products[u]
                running[q + 1] = total
            return carry

        lax.fori_loop(0, pairs // UNROLL, group, 0)
        for half in range(2):
            for u in range(n):
                r = half * n + u
                finish(r, running[table[2 * LAST + s, block(r)]])
            if between is not None and half == 0:
                between()

    def cross(source, slot, send, recv, peer):
        return pltpu.make_async_remote_copy(
            src_ref=source,
            dst_ref=slot,
            send_sem=send.at[peer],
            recv_sem=recv.at[me],
            device_id={"snap": peer},
            device_id_type=MESH,
        )

    def even_copy(peer):
        return cross(conv.at[0, peer], xbuf.at[0, 2 * me], send_even, recv_even, peer)

    def odd_copy(peer):
        return cross(conv.at[1, peer], xbuf.at[0, 2 * me + 1], send_odd, recv_odd, peer)

    def rest_copy(peer):
        return cross(
            conv.at[:, n + peer], xbuf.at[1, pl.ds(2 * me, 2)], send_rest, recv_rest, peer
        )

    def landed(slot, semaphore):
        pltpu.make_async_copy(slot, slot, semaphore).wait()

    def sort_tiles():
        shape = (tiles, ranks.shape[1])
        lane = lax.broadcasted_iota(jnp.int32, shape, 1)
        sub = lax.broadcasted_iota(jnp.int32, shape, 0)
        square = (tiles, tiles)
        lane_sq = lax.broadcasted_iota(jnp.int32, square, 1)
        sub_sq = lax.broadcasted_iota(jnp.int32, square, 0)

        def upright(line):
            wide = jnp.broadcast_to(line, square)
            return jnp.sum(jnp.where(lane_sq == sub_sq, wide, 0), axis=1, keepdims=True)

        def pick(column, chosen):
            return jnp.sum(jnp.where(chosen, column, 0), axis=0, keepdims=True)

        few = (blocks, blocks)
        lane_few = lax.broadcasted_iota(jnp.int32, few, 1)
        sub_few = lax.broadcasted_iota(jnp.int32, few, 0)
        lane_line = lax.broadcasted_iota(jnp.int32, (1, ranks.shape[1]), 1)

        def line_at(kind, value):
            ranks[kind : kind + 1, :] = value

        def unlisted(index):
            value = jnp.ones_like(index)
            for i in range(2 * bound):
                value = jnp.where(index == lists[i, vert], 0, value)
            return value * blocks + index

        key_up = unlisted(lax.broadcasted_iota(jnp.int32, (blocks, ranks.shape[1]), 0))
        key_line = unlisted(lane_line)
        place_line = jnp.sum(jnp.where(key_up < key_line, 1, 0), axis=0, keepdims=True)
        line_at(PLACE, place_line)
        smaller = jnp.where(unlisted(lane_few) < unlisted(sub_few), 1, 0)
        place = jnp.sum(smaller, axis=1, keepdims=True)
        wide = (blocks, ranks.shape[1])
        line_at(
            BLOCK,
            pick(
                lax.broadcasted_iota(jnp.int32, wide, 0),
                place == lax.broadcasted_iota(jnp.int32, wide, 1),
            ),
        )
        for s in range(rows.shape[0]):
            row_line = rows[s : s + 1, :]
            row = upright(row_line)
            col = upright(cols[s : s + 1, :])
            earlier = jnp.where(lane_sq < sub_sq, 1, 0)
            alike = jnp.where(jnp.broadcast_to(row_line, square) == row, earlier, 0)
            within = jnp.sum(alike, axis=1, keepdims=True)
            found = pick(jnp.ones_like(row), row == lane)
            padded = found + (found & 1)
            base = jnp.sum(jnp.where(lane < row, padded, 0), axis=1, keepdims=True)
            spot = base + within
            moved = jnp.where(lane == col - bound, place_line, 0)
            moved = jnp.sum(moved, axis=1, keepdims=True) + bound
            inner = jnp.where(col >= bound, jnp.where(col < bound + blocks, 1, 0), 0)
            again = jnp.where(inner == 1, moved, col)
            for side in range(2):
                chosen = spot == 2 * lane + side
                count = pick(jnp.ones_like(row), chosen)
                line_at(2 * (ORDER + side) + s, jnp.where(count > 0, pick(sub, chosen), tiles))
                line_at(2 * (COLUMN + side) + s, pick(col, chosen))
                line_at(2 * (AGAIN + side) + s, pick(again, chosen))
            line = pick(row, spot == 2 * lane)
            same = jnp.where(line == pltpu.roll(line, 1, axis=1), 1, 0)
            line_at(2 * KEEP + s, jnp.where(lane_line == 0, 0, same))
            wide_pad = jnp.broadcast_to(padded, wide)
            wide_lane = lax.broadcasted_iota(jnp.int32, wide, 1)
            wide_sub = lax.broadcasted_iota(jnp.int32, wide, 0)
            pad = jnp.sum(jnp.where(wide_lane == wide_sub, wide_pad, 0), axis=1, keepdims=True)
            upto = jnp.sum(jnp.where(wide_sub <= wide_lane, pad, 0), axis=0, keepdims=True)
            line_at(2 * LAST + s, jnp.where(found > 0, upto >> 1, 0))
        return pltpu.make_async_copy(ranks, table, sort_sem)

    tiny[0].wait()
    running[0] = jnp.zeros_like(running[0])
    for tile in (tile0, tile1):
        tile[tiles] = jnp.zeros_like(tile[tiles])
    loads[0].wait()
    loads[1].wait()
    for copy in loads[2:] + tiny[1:]:
        copy.start()
    make_pack(lambda b: feat0[b], weights1, pack0)
    pl.semaphore_wait(barrier, n + 1)
    halo0 = halo_copies(pack0, ext0, 0)
    for copy in halo0:
        copy.start()
    loads[2].wait()
    make_pack(lambda b: feat1[b], weights1, pack1)
    halo1 = halo_copies(pack1, ext1, 1)
    for copy in halo1:
        copy.start()
    for copy in tiny[1:]:
        copy.wait()
    sorting = sort_tiles()
    sorting.start()
    project_own(lambda i: feat0[i], blocks, weights1, ext0, bound)

    def keep_conv(s):
        def finish(r, total):
            conv[s, r] = jnp.maximum(total, 0.0).astype(jnp.bfloat16)

        return finish

    sorting.wait()
    loads[3].wait()
    for copy in halo0:
        copy.wait_recv()

    def send_evens():
        for d in offsets:
            even_copy(lax.rem(me + d, n)).start()
        pltpu.make_async_copy(conv.at[0, me], xbuf.at[0, 2 * me], recv_even.at[me]).start()

    convolve(0, COLUMN, ext0, tile0, lambda p: table[BLOCK, p], keep_conv(0), send_evens)
    project_own(lambda i: feat1[i], blocks, weights1, ext1, bound)
    loads[4].wait()
    for copy in halo1:
        copy.wait_recv()
    convolve(1, COLUMN, ext1, tile1, lambda p: table[BLOCK, p], keep_conv(1))
    for d in offsets:
        odd_copy(lax.rem(me + d, n)).start()
    pltpu.make_async_copy(conv.at[1, me], xbuf.at[0, 2 * me + 1], recv_odd.at[me]).start()
    for d in offsets:
        rest_copy(lax.rem(me + d, n)).start()
    pltpu.make_async_copy(
        conv.at[:, n + me], xbuf.at[1, pl.ds(2 * me, 2)], recv_rest.at[me]
    ).start()

    for copy in loads[5:]:
        copy.wait()

    def cell(x, hidden, memory, layer):
        gates = (
            jnp.dot(x, weights[layer, :width], preferred_element_type=jnp.float32)
            + jnp.dot(hidden[...], weights[layer, width:], preferred_element_type=jnp.float32)
            + bias[layer][None, :]
        )
        kept = sigmoid(gates[:, width : 2 * width]) * memory[...]
        new = kept + sigmoid(gates[:, :width]) * jnp.tanh(gates[:, 2 * width : 3 * width])
        memory[...] = new
        result = (sigmoid(gates[:, 3 * width :]) * jnp.tanh(new)).astype(jnp.bfloat16)
        hidden[...] = result
        return result

    lates = (late0, late1)

    def early_copy(owner):
        return cross(
            hbuf.at[0, pl.ds(2 * owner, 2)], early.at[me], send_early, recv_early, owner
        )

    def late_copy(part, owner):
        return cross(
            hbuf.at[1, 2 * owner + part], lates[part].at[me],
            send_late.at[part], recv_late.at[part], owner,
        )

    for half in range(2):
        h0[...] = jnp.zeros_like(h0)
        h1[...] = jnp.zeros_like(h1)
        c0[...] = jnp.zeros_like(c0)
        c1[...] = jnp.zeros_like(c1)

        def step(owner, carry, half=half):
            if half == 0:
                landed(xbuf.at[0, 2 * owner], recv_even.at[owner])
                landed(xbuf.at[0, 2 * owner + 1], recv_odd.at[owner])
            else:
                landed(xbuf.at[1, pl.ds(2 * owner, 2)], recv_rest.at[owner])
            for part in range(2):
                t = 2 * owner + part
                low = cell(xbuf[half, t], h0, c0, 0)
                hbuf[half, t] = cell(low, h1, c1, 1)
            return carry

        lax.fori_loop(0, n, step, 0)
        if half == 0:
            for d in offsets:
                early_copy(lax.rem(me + d, n)).start()
            pltpu.make_async_copy(
                hbuf.at[0, pl.ds(2 * me, 2)], early.at[me], recv_early.at[me]
            ).start()
        else:
            for part in range(2):
                for d in offsets:
                    late_copy(part, lax.rem(me + d, n)).start()
                pltpu.make_async_copy(
                    hbuf.at[1, 2 * me + part], lates[part].at[me], recv_late.at[part, me]
                ).start()

    def arrive(slots, semaphore):
        def one(source, carry):
            landed(slots.at[source], semaphore.at[source])
            return carry

        lax.fori_loop(0, n, one, 0)

    def drain(i, carry):
        peer = lax.rem(me + i, n)
        even_copy(peer).wait_send()
        odd_copy(peer).wait_send()
        rest_copy(peer).wait_send()
        early_copy(peer).wait_send()
        late_copy(0, peer).wait_send()
        return carry

    packs, wides, grids = (pack2, pack3), (ext2, ext3), (tile0, tile1)
    halos = []
    arrive(early, recv_early)
    for part in range(2):
        make_pack(
            lambda b, part=part: early[table[PLACE, b], part], weights2, packs[part]
        )
        copies = halo_copies(packs[part], wides[part], 2 + part)
        for copy in copies:
            copy.start()
        halos.append(copies)
    for part in range(2):
        project_own(lambda i, part=part: early[i, part], n, weights2, wides[part], bound)
    for part in range(2):
        if part == 1:
            lax.fori_loop(1, n, drain, 0)
            for copies in [halo0, halo1] + halos:
                for copy in copies:
                    copy.wait_send()
        for copy in halos[part]:
            copy.wait_recv()
        arrive(lates[part], recv_late.at[part])
        project_own(
            lambda i, part=part: lates[part][i], n, weights2, wides[part], bound + n
        )

        def finish(r, total, part=part):
            out[part, r] = total.astype(jnp.bfloat16)

        convolve(part, AGAIN, wides[part], grids[part], lambda r: r, finish)

    def last(i, carry):
        late_copy(1, lax.rem(me + i, n)).wait_send()
        return carry

    lax.fori_loop(1, n, last, 0)


def whole(send_lists, tile_rows, tile_cols, features, tile_vals, w1, w2, lstm_weight, lstm_bias):
    n = lax.axis_size("snap")
    snaps, blocks, _, width = features.shape
    bound = send_lists.shape[0] // 2
    tiles = tile_vals.shape[1]
    total = snaps * n
    hbm = pl.BlockSpec(memory_space=pltpu.HBM)

    def rows(count, dtype=jnp.bfloat16):
        return pltpu.VMEM((count, BS, width), dtype)

    def states(dtype):
        return pltpu.VMEM((BS, width), dtype)

    dma = pltpu.SemaphoreType.DMA
    operands = [
        pltpu.with_memory_space_constraint(x, pltpu.HBM)
        for x in (
            send_lists, tile_rows, tile_cols, features, tile_vals, w1, w2, lstm_weight, lstm_bias
        )
    ]
    return pl.pallas_call(
        functools.partial(whole_kernel, n),
        out_shape=jax.ShapeDtypeStruct(features.shape, jnp.bfloat16),
        in_specs=[hbm] * 9,
        out_specs=pl.BlockSpec(memory_space=pltpu.VMEM),
        scratch_shapes=[
            pltpu.SMEM(send_lists.shape, jnp.int32), pltpu.VMEM(tile_rows.shape, jnp.int32),
            pltpu.VMEM(tile_cols.shape, jnp.int32),
            pltpu.VMEM((24, 128), jnp.int32), pltpu.SMEM((24, 128), jnp.int32),
            rows(blocks), rows(blocks),
            pltpu.VMEM((tiles + 1, BS, BS), jnp.bfloat16),
            pltpu.VMEM((tiles + 1, BS, BS), jnp.bfloat16),
            rows(blocks + 2 * bound), rows(blocks + 2 * bound),
            rows(blocks + 2 * bound), rows(blocks + 2 * bound),
            rows(2 * bound), rows(2 * bound), rows(2 * bound), rows(2 * bound),
            rows((tiles + blocks) // 2 + 1, jnp.float32),
            pltpu.VMEM((snaps, blocks, BS, width), jnp.bfloat16),
            pltpu.VMEM((2, total, BS, width), jnp.bfloat16),
            pltpu.VMEM((2, total, BS, width), jnp.bfloat16),
            pltpu.VMEM((n, 2, BS, width), jnp.bfloat16), rows(n), rows(n),
            pltpu.VMEM(w1.shape, jnp.bfloat16), pltpu.VMEM(w2.shape, jnp.bfloat16),
            pltpu.VMEM(lstm_weight.shape, jnp.bfloat16), pltpu.VMEM(lstm_bias.shape, jnp.float32),
            states(jnp.bfloat16), states(jnp.float32), states(jnp.bfloat16), states(jnp.float32),
            dma((8,)), dma((3,)), dma(()), dma((4, 2)), dma((4, 2)),
            dma((n,)), dma((n,)), dma((n,)), dma((n,)), dma((n,)), dma((n,)),
            dma((n,)), dma((n,)), dma((2, n)), dma((2, n)),
        ],
        compiler_params=pltpu.CompilerParams(
            collective_id=0, has_side_effects=True, vmem_limit_bytes=44 * 2**20
        ),
        cost_estimate=pl.CostEstimate(
            flops=12 << 30, bytes_accessed=11 << 20, transcendentals=42 << 20
        ),
        name="whole",
    )(*operands)


def shards(
    features,
    tile_rows,
    tile_cols,
    tile_vals,
    send_lists,
    conv1_weight,
    conv2_weight,
    lstm_weight,
    lstm_bias,
):
    snapshots, vertices, width = features.shape
    own = features.reshape(snapshots, vertices // BS, BS, width)
    mixed = whole(
        send_lists.T, tile_rows, tile_cols, own, tile_vals,
        conv1_weight, conv2_weight, lstm_weight, lstm_bias,
    )
    return mixed.reshape(snapshots, vertices, width)


def solution(mesh):
    placed = (
        P("snap", "vert", None),
        P("snap", "vert"),
        P("snap", "vert"),
        P("snap", "vert", None, None),
        P(),
        P(),
        P(),
        P(),
        P(),
    )
    return jax.shard_map(
        shards, mesh=mesh, in_specs=placed, out_specs=P("snap", "vert", None), check_vma=False
    )
```
